8 devices in a mesh: rep: 1 (over z), mp: 2 (over y), tok: 4 (over x, core).
Axes of the slice: x: 2, y: 2, z: 1, core: 2. Of those that a mesh axis runs over, the one named last changes fastest.
Arguments:
- x_in: bfloat16 [2, 4096, 3584], P(None, ('rep', 'tok', 'mp'))
- seg_ids: int32 [2, 4096], P(None, ('rep', 'tok', 'mp'))
- g_attn: bfloat16 [2, 3584], replicated
- w_q: bfloat16 [2, 3584, 16, 256], P(None, 'tok', 'mp')
- w_k: bfloat16 [2, 3584, 8, 256], P(None, 'tok', 'mp')
- w_v: bfloat16 [2, 3584, 8, 256], P(None, 'tok', 'mp')
- w_o: bfloat16 [2, 16, 256, 3584], P(None, 'mp', None, 'tok')
- g_mlp: bfloat16 [2, 3584], replicated
- w_gate: bfloat16 [2, 3584, 14336], P(None, 'tok', 'mp')
- w_up: bfloat16 [2, 3584, 14336], P(None, 'tok', 'mp')
- w_down: bfloat16 [2, 14336, 3584], P(None, 'mp', 'tok')
Outputs:
- output: float32 [2, 4096, 3584], P(None, ('rep', 'tok', 'mp'))
All inputs are finite; a program needn't handle non-finite values.
Results may differ from the reference program's by a relative error of at most 0.00833919.
Values are sent between devices in bfloat16 or wider.
A program may use at most 1 GiB of HBM per device.

```python
import jax
import jax.numpy as jnp
from jax import lax

EMBED_DIM = 3584
FFN_DIM = 14336
Q_HEADS = 16
KV_HEADS = 8
HEAD_DIM = 256
LAYERS = 2
MICRO_BATCHES = 2
NUM_SHARDS = 4
BLOCK_LEN = 1024
CUT_COUNT = 2
WAVE_COUNT = 4
TOKENS = NUM_SHARDS * BLOCK_LEN
BLOCKS = MICRO_BATCHES * NUM_SHARDS
NORM_EPS = 1e-5
ROPE_BASE = 10000.0
NEG_BIG = -1e30


def draw_segments(seg_key):
    cut_at = jax.random.randint(seg_key, (BLOCKS, CUT_COUNT), 1, BLOCK_LEN, dtype=jnp.int32)
    tok_order = jnp.arange(BLOCK_LEN, dtype=jnp.int32)
    is_start = jnp.any(tok_order[None, None, :] == cut_at[:, :, None], axis=1) | (tok_order[None, :] == 0)
    local_ids = jnp.cumsum(is_start.astype(jnp.int32), axis=1) - 1
    base_ids = jnp.arange(BLOCKS, dtype=jnp.int32)[:, None] * BLOCK_LEN
    return (local_ids + base_ids).astype(jnp.int32).reshape(MICRO_BATCHES, TOKENS)


def setup_inputs(seed: int = 0, part: int = 0) -> dict:
    root_key = jax.random.key(seed)
    key_list = jax.random.split(root_key, 12)
    part_key = jax.random.fold_in(key_list[0], part)
    noise_key, cos_key, sin_key, seg_key = jax.random.split(part_key, 4)
    freq_n = jnp.arange(1, WAVE_COUNT + 1, dtype=jnp.float32)
    t_frac = jnp.arange(BLOCK_LEN, dtype=jnp.float32) / BLOCK_LEN
    angles = 2.0 * jnp.pi * freq_n[:, None] * t_frac[None, :]
    amp_cos = jax.random.normal(cos_key, (BLOCKS, WAVE_COUNT, EMBED_DIM), jnp.float32)
    amp_sin = jax.random.normal(sin_key, (BLOCKS, WAVE_COUNT, EMBED_DIM), jnp.float32)
    smooth = (jnp.einsum('ks,bke->bse', jnp.cos(angles), amp_cos) + jnp.einsum('ks,bke->bse', jnp.sin(angles), amp_sin)) * WAVE_COUNT ** -0.5
    noise = jax.random.normal(noise_key, (BLOCKS, BLOCK_LEN, EMBED_DIM), jnp.float32)
    x_in = (0.8 * smooth + 0.6 * noise).reshape(MICRO_BATCHES, TOKENS, EMBED_DIM).astype(jnp.bfloat16)

    def weight(wkey, shape, fan_in):
        return (jax.random.normal(wkey, shape, jnp.float32) * fan_in ** -0.5).astype(jnp.bfloat16)

    def gains(wkey):
        return jax.random.uniform(wkey, (LAYERS, EMBED_DIM), jnp.float32, minval=0.5, maxval=1.5).astype(jnp.bfloat16)

    return {
        'x_in': x_in,
        'seg_ids': draw_segments(seg_key),
        'g_attn': gains(key_list[1]),
        'w_q': weight(key_list[2], (LAYERS, EMBED_DIM, Q_HEADS, HEAD_DIM), EMBED_DIM),
        'w_k': weight(key_list[3], (LAYERS, EMBED_DIM, KV_HEADS, HEAD_DIM), EMBED_DIM),
        'w_v': weight(key_list[4], (LAYERS, EMBED_DIM, KV_HEADS, HEAD_DIM), EMBED_DIM),
        'w_o': weight(key_list[5], (LAYERS, Q_HEADS, HEAD_DIM, EMBED_DIM), Q_HEADS * HEAD_DIM),
        'g_mlp': gains(key_list[6]),
        'w_gate': weight(key_list[7], (LAYERS, EMBED_DIM, FFN_DIM), EMBED_DIM),
        'w_up': weight(key_list[8], (LAYERS, EMBED_DIM, FFN_DIM), EMBED_DIM),
        'w_down': weight(key_list[9], (LAYERS, FFN_DIM, EMBED_DIM), FFN_DIM),
    }


def rms_norm(resid, gain_vec):
    mean_sq = jnp.mean(resid * resid, axis=-1, keepdims=True)
    return (resid * lax.rsqrt(mean_sq + NORM_EPS) * gain_vec.astype(jnp.float32)).astype(jnp.bfloat16)


def seg_positions(seg_rows):
    positions = jnp.arange(seg_rows.shape[-1], dtype=jnp.int32)
    previous = jnp.concatenate([seg_rows[..., :1] - 1, seg_rows[..., :-1]], axis=-1)
    start_at = jnp.where(seg_rows != previous, positions, 0)
    return positions - lax.cummax(start_at, axis=seg_rows.ndim - 1)


def rope_tables(positions, head_dim):
    half_dim = head_dim // 2
    inv_freq = ROPE_BASE ** (-2.0 * jnp.arange(half_dim, dtype=jnp.float32) / head_dim)
    angles = positions.astype(jnp.float32)[..., None] * inv_freq
    return jnp.cos(angles), jnp.sin(angles)


def apply_rope(values, cos_t, sin_t):
    half_dim = values.shape[-1] // 2
    first_half = values[..., :half_dim]
    second_half = values[..., half_dim:]
    return jnp.concatenate([first_half * cos_t - second_half * sin_t, second_half * cos_t + first_half * sin_t], axis=-1)


def block_attention(operands):
    q_blk, k_blk, v_blk, seg_blk = operands
    tok_order = jnp.arange(BLOCK_LEN)
    allowed = (seg_blk[:, None] == seg_blk[None, :]) & (tok_order[None, :] <= tok_order[:, None])

    def one_group(group_ops):
        q_grp, k_grp, v_grp = group_ops
        scores = jnp.einsum('sgd,td->sgt', q_grp.astype(jnp.float32), k_grp.astype(jnp.float32)) * HEAD_DIM ** -0.5
        scores = jnp.where(allowed[:, None, :], scores, NEG_BIG)
        probs_bf = jax.nn.softmax(scores, axis=-1).astype(jnp.bfloat16)
        return jnp.einsum('sgt,td->sgd', probs_bf.astype(jnp.float32), v_grp.astype(jnp.float32)).astype(jnp.bfloat16)

    group_out = lax.map(one_group, (jnp.moveaxis(q_blk, 1, 0), jnp.moveaxis(k_blk, 1, 0), jnp.moveaxis(v_blk, 1, 0)))
    return jnp.moveaxis(group_out, 0, 1)


def reference(x_in, seg_ids, g_attn, w_q, w_k, w_v, w_o, g_mlp, w_gate, w_up, w_down):
    groups = Q_HEADS // KV_HEADS
    seg_blocks = seg_ids.reshape(BLOCKS, BLOCK_LEN)
    cos_t, sin_t = rope_tables(seg_positions(seg_blocks), HEAD_DIM)
    cos_t = cos_t[:, :, None, :]
    sin_t = sin_t[:, :, None, :]

    def layer_step(residual, layer_w):
        ga_vec, wq_l, wk_l, wv_l, wo_l, gm_vec, wg_l, wu_l, wd_l = layer_w
        hidden = rms_norm(residual, ga_vec).reshape(BLOCKS, BLOCK_LEN, EMBED_DIM).astype(jnp.float32)
        q_lin = jnp.einsum('bse,end->bsnd', hidden, wq_l.astype(jnp.float32))
        k_lin = jnp.einsum('bse,end->bsnd', hidden, wk_l.astype(jnp.float32))
        v_lin = jnp.einsum('bse,end->bsnd', hidden, wv_l.astype(jnp.float32))
        q_rot = apply_rope(q_lin, cos_t, sin_t).astype(jnp.bfloat16).reshape(BLOCKS, BLOCK_LEN, KV_HEADS, groups, HEAD_DIM)
        k_rot = apply_rope(k_lin, cos_t, sin_t).astype(jnp.bfloat16)
        v_val = v_lin.astype(jnp.bfloat16)
        attn_out = lax.map(block_attention, (q_rot, k_rot, v_val, seg_blocks))
        attn_out = attn_out.reshape(BLOCKS, BLOCK_LEN, Q_HEADS, HEAD_DIM).astype(jnp.float32)
        proj_out = jnp.einsum('bsnd,nde->bse', attn_out, wo_l.astype(jnp.float32))
        residual = residual + proj_out.reshape(MICRO_BATCHES, TOKENS, EMBED_DIM)
        hidden = rms_norm(residual, gm_vec).reshape(MICRO_BATCHES * TOKENS, EMBED_DIM)
        gate_val = jnp.dot(hidden, wg_l, preferred_element_type=jnp.float32)
        up_val = jnp.dot(hidden, wu_l, preferred_element_type=jnp.float32)
        act_val = (jax.nn.silu(gate_val) * up_val).astype(jnp.bfloat16)
        down_val = jnp.dot(act_val, wd_l, preferred_element_type=jnp.float32)
        return residual + down_val.reshape(MICRO_BATCHES, TOKENS, EMBED_DIM), None

    final_res, _ = lax.scan(layer_step, x_in.astype(jnp.float32), (g_attn, w_q, w_k, w_v, w_o, g_mlp, w_gate, w_up, w_down))
    return final_res
```

```python
import functools

import jax
import jax.numpy as jnp
from jax import lax
from jax.experimental import pallas as pl
from jax.experimental.pallas import tpu as pltpu
from jax.sharding import PartitionSpec as P


NORM_EPS = 1e-5
ROPE_BASE = 10000.0
NEG_BIG = -1e30
F32 = jnp.float32
BF16 = jnp.bfloat16
VMEM_LIMIT = 60 * 1024 * 1024


def seg_positions(seg_rows):
    positions = jnp.arange(seg_rows.shape[-1], dtype=jnp.int32)
    previous = jnp.concatenate([seg_rows[..., :1] - 1, seg_rows[..., :-1]], axis=-1)
    start_at = jnp.where(seg_rows != previous, positions, 0)
    return positions - lax.cummax(start_at, axis=seg_rows.ndim - 1)


def piece_dot(h_ref, piece_refs, whole_ref):
    depth = piece_refs[0].shape[0]
    for j, w_ref in enumerate(piece_refs):
        whole_ref[j * depth:(j + 1) * depth, :] = w_ref[...]
    return jnp.dot(h_ref[...], whole_ref[...], preferred_element_type=F32)


def proj_kernel(rope_tiles, head_dim, h_ref, *refs):
    piece_refs, (cos_ref, sin_ref, out_ref, whole_ref) = refs[:4], refs[4:]
    acc = piece_dot(h_ref, piece_refs, whole_ref)
    half = head_dim // 2

    def roped():
        cos_t, sin_t = cos_ref[...], sin_ref[...]
        for n in range(acc.shape[1] // head_dim):
            lo = n * head_dim
            a, b = acc[:, lo:lo + half], acc[:, lo + half:lo + head_dim]
            out_ref[:, lo:lo + half] = (a * cos_t - b * sin_t).astype(BF16)
            out_ref[:, lo + half:lo + head_dim] = (b * cos_t + a * sin_t).astype(BF16)

    def plain():
        out_ref[...] = acc.astype(BF16)

    if rope_tiles >= 1000:
        roped()
    else:
        tile = pl.program_id(0)
        pl.when(tile < rope_tiles)(roped)
        pl.when(tile >= rope_tiles)(plain)


def project(hidden, pieces, cos_t, sin_t, rope_cols, head_dim, tile=512):
    rows, feat = hidden.shape
    depth, cols = pieces[0].shape
    rope_tiles = 1000 if rope_cols == cols else rope_cols // tile
    return pl.pallas_call(
        functools.partial(proj_kernel, rope_tiles, head_dim),
        grid=(cols // tile,),
        in_specs=[pl.BlockSpec((rows, feat), lambda i: (0, 0))]
        + [pl.BlockSpec((depth, tile), lambda i: (0, i))] * 4
        + [pl.BlockSpec(cos_t.shape, lambda i: (0, 0))] * 2,
        out_specs=pl.BlockSpec((rows, tile), lambda i: (0, i)),
        out_shape=jax.ShapeDtypeStruct((rows, cols), BF16),
        scratch_shapes=[pltpu.VMEM((feat, tile), BF16)],
        compiler_params=pltpu.CompilerParams(vmem_limit_bytes=VMEM_LIMIT),
        cost_estimate=pl.CostEstimate(flops=2 * rows * feat * cols, bytes_accessed=2 * (rows * feat + feat * cols + rows * cols), transcendentals=0),
    )(hidden, *pieces, cos_t, sin_t)


def ffn_kernel(h_ref, *refs):
    out_ref, whole_gate, whole_up = refs[-3:]
    gate = piece_dot(h_ref, refs[0:4], whole_gate)
    up = piece_dot(h_ref, refs[4:8], whole_up)
    out_ref[...] = (gate * jax.nn.sigmoid(gate) * up).astype(BF16)


def ffn_chunk(hidden, pieces, act_buf, total_cols, first_col, tile=256):
    rows, feat = hidden.shape
    depth, both = pieces[0].shape
    cols = both // 2
    steps, base = cols // tile, first_col // tile
    gate_spec = pl.BlockSpec((depth, tile), lambda i: (0, i))
    up_spec = pl.BlockSpec((depth, tile), lambda i: (0, steps + i))
    in_specs = [pl.BlockSpec((rows, feat), lambda i: (0, 0))] + [gate_spec] * 4 + [up_spec] * 4
    operands = [hidden, *pieces, *pieces]
    aliases = {}
    if act_buf is not None:
        in_specs.append(pl.BlockSpec(memory_space=pl.ANY))
        operands.append(act_buf)
        aliases = {9: 0}
    return pl.pallas_call(
        ffn_kernel,
        grid=(steps,),
        in_specs=in_specs,
        out_specs=pl.BlockSpec((rows, tile), lambda i: (0, base + i)),
        out_shape=jax.ShapeDtypeStruct((rows, total_cols), BF16),
        input_output_aliases=aliases,
        scratch_shapes=[pltpu.VMEM((feat, tile), BF16)] * 2,
        compiler_params=pltpu.CompilerParams(vmem_limit_bytes=VMEM_LIMIT),
        cost_estimate=pl.CostEstimate(flops=4 * rows * feat * cols, bytes_accessed=2 * (rows * feat + 2 * feat * cols + rows * cols), transcendentals=rows * cols),
    )(*operands)


def attn_kernel(head_dim, q_ref, ka_ref, va_ref, kb_ref, vb_ref, lo_ref, hi_ref, ia_ref, ib_ref, out_ref):
    lo, hi = lo_ref[0], hi_ref[0]
    ok_a = (ia_ref[...] >= lo) & (ia_ref[...] <= hi)
    ok_b = (ib_ref[...] >= lo) & (ib_ref[...] <= hi)
    dims = (((1,), (1,)), ((), ()))
    scale = head_dim ** -0.5
    for g in range(q_ref.shape[2] // head_dim):
        q = q_ref[0, :, g * head_dim:(g + 1) * head_dim]
        s_a = jnp.where(ok_a, lax.dot_general(q, ka_ref[0], dims, preferred_element_type=F32) * scale, NEG_BIG)
        s_b = jnp.where(ok_b, lax.dot_general(q, kb_ref[0], dims, preferred_element_type=F32) * scale, NEG_BIG)
        top = jnp.maximum(jnp.max(s_a, axis=1, keepdims=True), jnp.max(s_b, axis=1, keepdims=True))
        e_a, e_b = jnp.exp(s_a - top), jnp.exp(s_b - top)
        inv = 1.0 / (jnp.sum(e_a, axis=1, keepdims=True) + jnp.sum(e_b, axis=1, keepdims=True))
        out = jnp.dot((e_a * inv).astype(BF16), va_ref[0], preferred_element_type=F32)
        out = out + jnp.dot((e_b * inv).astype(BF16), vb_ref[0], preferred_element_type=F32)
        out_ref[0, :, g * head_dim:(g + 1) * head_dim] = out.astype(BF16)


def attention(q, kv_a, kv_b, lo, hi, idx_a, idx_b, head_dim):
    micro_n, rows, q_cols = q.shape
    kv_heads = kv_a.shape[2] // head_dim // 2
    group = q_cols // kv_heads
    k_spec = pl.BlockSpec((1, rows, head_dim), lambda m, n: (m, 0, n))
    v_spec = pl.BlockSpec((1, rows, head_dim), lambda m, n: (m, 0, kv_heads + n))
    q_spec = pl.BlockSpec((1, rows, group), lambda m, n: (m, 0, n))
    col_spec = pl.BlockSpec((1, rows, 1), lambda m, n: (m, 0, 0))
    row_spec = pl.BlockSpec((1, rows), lambda m, n: (0, 0))
    return pl.pallas_call(
        functools.partial(attn_kernel, head_dim),
        grid=(micro_n, kv_heads),
        in_specs=[q_spec, k_spec, v_spec, k_spec, v_spec, col_spec, col_spec, row_spec, row_spec],
        out_specs=q_spec,
        out_shape=jax.ShapeDtypeStruct(q.shape, BF16),
        compiler_params=pltpu.CompilerParams(vmem_limit_bytes=VMEM_LIMIT),
        cost_estimate=pl.CostEstimate(flops=16 * micro_n * rows * rows * q_cols, bytes_accessed=8 * micro_n * rows * q_cols, transcendentals=2 * micro_n * rows * rows * q_cols // head_dim),
    )(q, kv_a, kv_a, kv_b, kv_b, lo, hi, idx_a, idx_b)


def after(value, *earlier):
    return lax.optimization_barrier((value, *earlier))[0] if earlier else value


def norm_pieces(pieces, gains):
    feat = sum(p.shape[1] for p in pieces)
    total = sum(jnp.sum(p * p, axis=1, keepdims=True) for p in pieces)
    inv = lax.rsqrt(total / feat + NORM_EPS)
    return jnp.concatenate([(p * inv * g).astype(BF16) for p, g in zip(pieces, gains)], axis=1)


X_ORDER = (
    ('kv', 0, 0), ('q', 0, 0), ('o', 0, 0), ('g', 0, 0), ('g', 0, 1), ('g', 0, 2), ('g', 0, 3),
    ('d', 0, 0), ('d', 0, 1), ('kv', 1, 0), ('q', 1, 0), ('o', 1, 0), ('g', 1, 0), ('g', 1, 1), ('g', 1, 2), ('g', 1, 3),
    ('d', 1, 0), ('d', 1, 1),
)


FFN_CHUNKS = ((2048, 2048, 2048, 1024),) * 2
FAR_FROM = (1, 1)
DOWN_CHUNKS = ((512, 384), (512, 384))


def solution(mesh):
    act_spec = P(None, ('rep', 'tok', 'mp'), None)
    seg_spec = P(None, ('rep', 'tok', 'mp'))
    gain_spec = P(None, None)
    head_in = P(None, 'tok', 'mp', None)
    head_out = P(None, 'mp', None, 'tok')
    ffn_in = P(None, 'tok', 'mp')
    ffn_out = P(None, 'mp', 'tok')
    tok_n = mesh.shape['tok']
    over_x = [(i, i ^ 2) for i in range(tok_n)]
    over_core = [(i, i ^ 1) for i in range(tok_n)]

    def send_x(a):
        return lax.ppermute(a, 'tok', over_x)

    def send_core(a):
        return lax.ppermute(a, 'tok', over_core)

    def send_y(a):
        return lax.ppermute(a, 'mp', [(0, 1), (1, 0)])

    def first_part(own, order):
        k = len(order)
        order.append(k)
        return own, send_core(own), send_x(own), k

    def spread(parts, *earlier):
        own, near, cross, _ = parts
        cross = after(cross, *earlier)
        return own, near, cross, send_core(cross)

    def layer_pair(x_in, seg_ids, g_attn, w_q, w_k, w_v, w_o, g_mlp, w_gate, w_up, w_down):
        micro_n, part_len, feat = x_in.shape
        layers, depth = w_q.shape[0], w_q.shape[1]
        head_dim = w_q.shape[3]
        rows = micro_n * part_len
        ffn_cols = w_gate.shape[2]
        tok = lax.axis_index('tok')
        half_id = lax.axis_index('mp')

        def local_cols(a, axis):
            return [lax.dynamic_slice_in_dim(a, (tok ^ j) * depth, depth, axis) for j in range(4)]

        order = []
        firsts = [[sum(w[:c]) for c in range(len(w))] for w in FFN_CHUNKS]

        def own_piece(kind, l, c):
            if kind == 'kv':
                return jnp.concatenate([w_k[l].reshape(depth, -1), w_v[l].reshape(depth, -1)], axis=1)
            if kind == 'q':
                return w_q[l].reshape(depth, -1)
            if kind == 'o':
                return w_o[l].reshape(-1, depth)
            if kind == 'g':
                at = slice(firsts[l][c], firsts[l][c] + FFN_CHUNKS[l][c])
                return jnp.concatenate([w_gate[l, :, at], w_up[l, :, at]], axis=1)
            at = sum(DOWN_CHUNKS[l][:c])
            return w_down[l, :, at:at + DOWN_CHUNKS[l][c]]

        parts = {key: first_part(own_piece(*key), order) for key in X_ORDER}
        plans = [
            (
                parts['kv', l, 0], parts['q', l, 0], parts['o', l, 0],
                [parts['g', l, c] for c in range(len(FFN_CHUNKS[l]))],
                [parts['d', l, c] for c in range(len(DOWN_CHUNKS[l]))],
            )
            for l in range(layers)
        ]

        x_own = jnp.concatenate(local_cols(x_in.reshape(rows, feat), 1), axis=1)
        seg_far = send_y(seg_ids)
        x_far = send_y(after(x_own, seg_far))
        first_half = jnp.where(half_id == 0, seg_ids, seg_far)
        second_half = jnp.where(half_id == 0, seg_far, seg_ids)
        positions = seg_positions(jnp.concatenate([first_half, second_half], axis=1))
        idx = jnp.arange(part_len, dtype=jnp.int32)
        at_own = half_id * part_len
        at_far = (1 - half_id) * part_len
        inv_freq = ROPE_BASE ** (-2.0 * jnp.arange(head_dim // 2, dtype=F32) / head_dim)

        def tables(at):
            pos = lax.dynamic_slice_in_dim(positions, at, part_len, 1)
            hi = jnp.broadcast_to((idx + at)[None, :], pos.shape)
            angles = (pos.astype(F32)[..., None] * inv_freq).reshape(rows, -1)
            return jnp.cos(angles), jnp.sin(angles), (hi - pos)[..., None], hi[..., None], (idx + at)[None, :]

        cos_own, sin_own, lo_own, hi_own, idx_own = tables(at_own)
        cos_far, sin_far, lo_far, hi_far, idx_far = tables(at_far)

        resid = [x_own[:, j * depth:(j + 1) * depth].astype(F32) for j in range(4)]
        shape3 = (micro_n, part_len, -1)
        k_cols = plans[0][0][0].shape[1] // 2
        q_cols = plans[0][1][0].shape[1]
        gate_q = ()
        out = jnp.zeros((rows, feat), F32)
        y_next = send_y(after(plans[0][2][0], x_far))
        for l in range(layers):
            kv_w, q_w, o_w, gu_w, d_w = plans[l]
            gains = [g.astype(F32)[None, :] for g in local_cols(g_attn[l], 0)]
            h_own = norm_pieces(resid, gains)
            if l == 0:
                h_far = norm_pieces([x_far[:, j * depth:(j + 1) * depth].astype(F32) for j in range(4)], gains)
            else:
                h_far = send_y(h_own)
            kv_w = spread(kv_w, *gate_q)
            q_w = spread(q_w, *gate_q)
            y_own = y_next
            kv_own = project(h_own, kv_w, cos_own, sin_own, k_cols, head_dim)
            q_own = project(h_own, q_w, cos_own, sin_own, q_cols, head_dim)
            o_w = spread(o_w, q_own)
            kv_far = project(h_far, kv_w, cos_far, sin_far, k_cols, head_dim)
            y_cross = send_y(after(o_w[2], (kv_far, h_far)[l]))
            q_far = project(h_far, q_w, cos_far, sin_far, q_cols, head_dim)
            o_y = (y_own, send_core(y_own), y_cross, send_core(y_cross))
            kv_own, q_own, kv_far, q_far = (a.reshape(shape3) for a in (kv_own, q_own, kv_far, q_far))
            o_far = attention(q_far, kv_own, kv_far, lo_far, hi_far, idx_own, idx_far, head_dim)
            o_got = send_y(o_far).reshape(rows, -1)
            o_own = attention(q_own, kv_own, kv_far, lo_own, hi_own, idx_own, idx_far, head_dim).reshape(rows, -1)
            base = [resid[j] + jnp.dot(o_own, o_w[j], preferred_element_type=F32) for j in range(4)]
            base = lax.optimization_barrier(base)
            resid = [base[j] + jnp.dot(o_got, o_y[j], preferred_element_type=F32) for j in range(4)]

            gains = [g.astype(F32)[None, :] for g in local_cols(g_mlp[l], 0)]
            h_own = norm_pieces(resid, gains)
            h_far = send_y(h_own)
            if l + 1 < layers:
                y_next = send_y(after(plans[l + 1][2][0], h_far))
            act_own = act_far = None
            starts = firsts[l]
            last_c = len(gu_w) - 1
            gate = (o_own, h_own)[l]
            pieces = []

            def far_chunk(c, gate, act_far):
                return ffn_chunk(after(h_far, gate), pieces[c], act_far, ffn_cols, starts[c])

            done_far = 0
            for c in range(len(gu_w)):
                pieces.append(spread(gu_w[c], gate))
                if c == last_c:
                    while done_far <= c:
                        gate = act_far = far_chunk(done_far, gate, act_far)
                        done_far += 1
                act_own = ffn_chunk(h_own, pieces[c], act_own, ffn_cols, starts[c])
                gate = act_own
                while FAR_FROM[l] <= c < last_c and done_far <= c:
                    gate = act_far = far_chunk(done_far, gate, act_far)
                    done_far += 1
            sums = []
            gate_d = ()
            for js in ((0, 1), (2, 3)):
                for c, parts_c in enumerate(d_w):
                    w4 = parts_c if js == (0, 1) else spread(parts_c, *gate_d)
                    at = sum(DOWN_CHUNKS[l][:c])
                    fars = []
                    for j in js:
                        far_sum = jnp.dot(act_far, w4[j], preferred_element_type=F32)
                        fars.append(far_sum)
                        got = send_y(far_sum)
                        mine = lax.optimization_barrier(jnp.dot(act_own, w4[j], preferred_element_type=F32))
                        sums.append((j, at, mine, got))
                    gate_d = (mine,) if js == (0, 1) else tuple(fars)
            gate_q = (sums[-1][2],)
            new_resid = [[] for _ in range(4)]
            for j, at, mine, got in sums:
                total = resid[j][:, at:at + mine.shape[1]] + mine + after(got, *gate_q)
                new_resid[j].append(total)
                if l + 1 == layers:
                    out = lax.dynamic_update_slice_in_dim(out, total, (tok ^ j) * depth + at, 1)
            resid = [jnp.concatenate(new_resid[j], axis=1) for j in range(4)]
        return out.reshape(micro_n, part_len, feat)

    return jax.shard_map(
        layer_pair,
        mesh=mesh,
        in_specs=(act_spec, seg_spec, gain_spec, head_in, head_in, head_in, head_out, gain_spec, ffn_in, ffn_in, ffn_out),
        out_specs=act_spec,
        check_vma=False,
    )
```

```python
import functools

import jax
import jax.numpy as jnp
from jax import lax
from jax.experimental import pallas as pl
from jax.experimental.pallas import tpu as pltpu
from jax.sharding import PartitionSpec as P


NORM_EPS = 1e-5
ROPE_BASE = 10000.0
NEG_BIG = -1e30
F32 = jnp.float32
BF16 = jnp.bfloat16
VMEM_LIMIT = 60 * 1024 * 1024


def seg_positions(seg_rows):
    positions = jnp.arange(seg_rows.shape[-1], dtype=jnp.int32)
    previous = jnp.concatenate([seg_rows[..., :1] - 1, seg_rows[..., :-1]], axis=-1)
    start_at = jnp.where(seg_rows != previous, positions, 0)
    return positions - lax.cummax(start_at, axis=seg_rows.ndim - 1)


def piece_dot(h_ref, piece_refs, whole_ref):
    depth = piece_refs[0].shape[0]
    for j, w_ref in enumerate(piece_refs):
        whole_ref[j * depth:(j + 1) * depth, :] = w_ref[...]
    return jnp.dot(h_ref[...], whole_ref[...], preferred_element_type=F32)


def proj_kernel(rope_tiles, head_dim, h_ref, *refs):
    piece_refs, (cos_ref, sin_ref, out_ref, whole_ref) = refs[:4], refs[4:]
    acc = piece_dot(h_ref, piece_refs, whole_ref)
    half = head_dim // 2

    def roped():
        cos_t, sin_t = cos_ref[...], sin_ref[...]
        for n in range(acc.shape[1] // head_dim):
            lo = n * head_dim
            a, b = acc[:, lo:lo + half], acc[:, lo + half:lo + head_dim]
            out_ref[:, lo:lo + half] = (a * cos_t - b * sin_t).astype(BF16)
            out_ref[:, lo + half:lo + head_dim] = (b * cos_t + a * sin_t).astype(BF16)

    def plain():
        out_ref[...] = acc.astype(BF16)

    if rope_tiles >= 1000:
        roped()
    else:
        tile = pl.program_id(0)
        pl.when(tile < rope_tiles)(roped)
        pl.when(tile >= rope_tiles)(plain)


def project(hidden, pieces, cos_t, sin_t, rope_cols, head_dim, tile=512):
    rows, feat = hidden.shape
    depth, cols = pieces[0].shape
    rope_tiles = 1000 if rope_cols == cols else rope_cols // tile
    return pl.pallas_call(
        functools.partial(proj_kernel, rope_tiles, head_dim),
        grid=(cols // tile,),
        in_specs=[pl.BlockSpec((rows, feat), lambda i: (0, 0))]
        + [pl.BlockSpec((depth, tile), lambda i: (0, i))] * 4
        + [pl.BlockSpec(cos_t.shape, lambda i: (0, 0))] * 2,
        out_specs=pl.BlockSpec((rows, tile), lambda i: (0, i)),
        out_shape=jax.ShapeDtypeStruct((rows, cols), BF16),
        scratch_shapes=[pltpu.VMEM((feat, tile), BF16)],
        compiler_params=pltpu.CompilerParams(vmem_limit_bytes=VMEM_LIMIT),
        cost_estimate=pl.CostEstimate(flops=2 * rows * feat * cols, bytes_accessed=2 * (rows * feat + feat * cols + rows * cols), transcendentals=0),
    )(hidden, *pieces, cos_t, sin_t)


def ffn_kernel(h_ref, *refs):
    out_ref, whole_gate, whole_up = refs[-3:]
    gate = piece_dot(h_ref, refs[0:4], whole_gate)
    up = piece_dot(h_ref, refs[4:8], whole_up)
    out_ref[...] = (gate * jax.nn.sigmoid(gate) * up).astype(BF16)


def ffn_chunk(hidden, pieces, act_buf, total_cols, first_col, tile=256):
    rows, feat = hidden.shape
    depth, both = pieces[0].shape
    cols = both // 2
    steps, base = cols // tile, first_col // tile
    gate_spec = pl.BlockSpec((depth, tile), lambda i: (0, i))
    up_spec = pl.BlockSpec((depth, tile), lambda i: (0, steps + i))
    in_specs = [pl.BlockSpec((rows, feat), lambda i: (0, 0))] + [gate_spec] * 4 + [up_spec] * 4
    operands = [hidden, *pieces, *pieces]
    aliases = {}
    if act_buf is not None:
        in_specs.append(pl.BlockSpec(memory_space=pl.ANY))
        operands.append(act_buf)
        aliases = {9: 0}
    return pl.pallas_call(
        ffn_kernel,
        grid=(steps,),
        in_specs=in_specs,
        out_specs=pl.BlockSpec((rows, tile), lambda i: (0, base + i)),
        out_shape=jax.ShapeDtypeStruct((rows, total_cols), BF16),
        input_output_aliases=aliases,
        scratch_shapes=[pltpu.VMEM((feat, tile), BF16)] * 2,
        compiler_params=pltpu.CompilerParams(vmem_limit_bytes=VMEM_LIMIT),
        cost_estimate=pl.CostEstimate(flops=4 * rows * feat * cols, bytes_accessed=2 * (rows * feat + 2 * feat * cols + rows * cols), transcendentals=rows * cols),
    )(*operands)


def attn_kernel(head_dim, q_ref, ka_ref, va_ref, kb_ref, vb_ref, lo_ref, hi_ref, ia_ref, ib_ref, out_ref):
    lo, hi = lo_ref[0], hi_ref[0]
    ok_a = (ia_ref[...] >= lo) & (ia_ref[...] <= hi)
    ok_b = (ib_ref[...] >= lo) & (ib_ref[...] <= hi)
    dims = (((1,), (1,)), ((), ()))
    scale = head_dim ** -0.5
    for g in range(q_ref.shape[2] // head_dim):
        q = q_ref[0, :, g * head_dim:(g + 1) * head_dim]
        s_a = jnp.where(ok_a, lax.dot_general(q, ka_ref[0], dims, preferred_element_type=F32) * scale, NEG_BIG)
        s_b = jnp.where(ok_b, lax.dot_general(q, kb_ref[0], dims, preferred_element_type=F32) * scale, NEG_BIG)
        top = jnp.maximum(jnp.max(s_a, axis=1, keepdims=True), jnp.max(s_b, axis=1, keepdims=True))
        e_a, e_b = jnp.exp(s_a - top), jnp.exp(s_b - top)
        inv = 1.0 / (jnp.sum(e_a, axis=1, keepdims=True) + jnp.sum(e_b, axis=1, keepdims=True))
        out = jnp.dot((e_a * inv).astype(BF16), va_ref[0], preferred_element_type=F32)
        out = out + jnp.dot((e_b * inv).astype(BF16), vb_ref[0], preferred_element_type=F32)
        out_ref[0, :, g * head_dim:(g + 1) * head_dim] = out.astype(BF16)


def attention(q, kv_a, kv_b, lo, hi, idx_a, idx_b, head_dim):
    micro_n, rows, q_cols = q.shape
    kv_heads = kv_a.shape[2] // head_dim // 2
    group = q_cols // kv_heads
    k_spec = pl.BlockSpec((1, rows, head_dim), lambda m, n: (m, 0, n))
    v_spec = pl.BlockSpec((1, rows, head_dim), lambda m, n: (m, 0, kv_heads + n))
    q_spec = pl.BlockSpec((1, rows, group), lambda m, n: (m, 0, n))
    col_spec = pl.BlockSpec((1, rows, 1), lambda m, n: (m, 0, 0))
    row_spec = pl.BlockSpec((1, rows), lambda m, n: (0, 0))
    return pl.pallas_call(
        functools.partial(attn_kernel, head_dim),
        grid=(micro_n, kv_heads),
        in_specs=[q_spec, k_spec, v_spec, k_spec, v_spec, col_spec, col_spec, row_spec, row_spec],
        out_specs=q_spec,
        out_shape=jax.ShapeDtypeStruct(q.shape, BF16),
        compiler_params=pltpu.CompilerParams(vmem_limit_bytes=VMEM_LIMIT),
        cost_estimate=pl.CostEstimate(flops=16 * micro_n * rows * rows * q_cols, bytes_accessed=8 * micro_n * rows * q_cols, transcendentals=2 * micro_n * rows * rows * q_cols // head_dim),
    )(q, kv_a, kv_a, kv_b, kv_b, lo, hi, idx_a, idx_b)


def after(value, *earlier):
    return lax.optimization_barrier((value, *earlier))[0] if earlier else value


def norm_pieces(pieces, gains):
    feat = sum(p.shape[1] for p in pieces)
    total = sum(jnp.sum(p * p, axis=1, keepdims=True) for p in pieces)
    inv = lax.rsqrt(total / feat + NORM_EPS)
    return jnp.concatenate([(p * inv * g).astype(BF16) for p, g in zip(pieces, gains)], axis=1)


X_ORDER = (
    ('kv', 0, 0), ('q', 0, 0), ('o', 0, 0), ('g', 0, 0), ('g', 0, 1), ('g', 0, 2), ('g', 0, 3),
    ('d', 0, 0), ('d', 0, 1), ('kv', 1, 0), ('q', 1, 0), ('o', 1, 0), ('g', 1, 0), ('g', 1, 1), ('g', 1, 2), ('g', 1, 3),
    ('d', 1, 0), ('d', 1, 1), ('d', 1, 2),
)


FFN_CHUNKS = ((2048, 2048, 2048, 1024),) * 2
DOWN_CHUNKS = ((512, 384), (384, 256, 256))
FFN_STEPS = (
    ('w0', 'w1', 'f0', 'f1', 'f2', 'w2', 'f3', 'w3'),
    ('w0', 'w1', 'f0', 'f1', 'f2', 'f3', 'w2', 'w3'),
)
DOWN_STEPS = (('o', 'f0', 'w0', 'f1', 'w1'), ('f0', 'o', 'f1', 'w0', 'w1', 'f2', 'w2'))


def solution(mesh):
    act_spec = P(None, ('rep', 'tok', 'mp'), None)
    seg_spec = P(None, ('rep', 'tok', 'mp'))
    gain_spec = P(None, None)
    head_in = P(None, 'tok', 'mp', None)
    head_out = P(None, 'mp', None, 'tok')
    ffn_in = P(None, 'tok', 'mp')
    ffn_out = P(None, 'mp', 'tok')
    tok_n = mesh.shape['tok']
    over_x = [(i, i ^ 2) for i in range(tok_n)]
    over_core = [(i, i ^ 1) for i in range(tok_n)]

    def send_x(a):
        return lax.ppermute(a, 'tok', over_x)

    def send_core(a):
        return lax.ppermute(a, 'tok', over_core)

    def send_y(a):
        return lax.ppermute(a, 'mp', [(0, 1), (1, 0)])

    def first_part(own, order):
        k = len(order)
        order.append(k)
        return own, send_core(own), send_x(own), k

    def spread(parts, *earlier):
        own, near, cross, _ = parts
        cross = after(cross, *earlier)
        return own, near, cross, send_core(cross)

    def layer_pair(x_in, seg_ids, g_attn, w_q, w_k, w_v, w_o, g_mlp, w_gate, w_up, w_down):
        micro_n, part_len, feat = x_in.shape
        layers, depth = w_q.shape[0], w_q.shape[1]
        head_dim = w_q.shape[3]
        rows = micro_n * part_len
        ffn_cols = w_gate.shape[2]
        tok = lax.axis_index('tok')
        half_id = lax.axis_index('mp')

        def local_cols(a, axis):
            return [lax.dynamic_slice_in_dim(a, (tok ^ j) * depth, depth, axis) for j in range(4)]

        order = []
        firsts = [[sum(w[:c]) for c in range(len(w))] for w in FFN_CHUNKS]

        def own_piece(kind, l, c):
            if kind == 'kv':
                return jnp.concatenate([w_k[l].reshape(depth, -1), w_v[l].reshape(depth, -1)], axis=1)
            if kind == 'q':
                return w_q[l].reshape(depth, -1)
            if kind == 'o':
                return w_o[l].reshape(-1, depth)
            if kind == 'g':
                at = slice(firsts[l][c], firsts[l][c] + FFN_CHUNKS[l][c])
                return jnp.concatenate([w_gate[l, :, at], w_up[l, :, at]], axis=1)
            at = sum(DOWN_CHUNKS[l][:c])
            return w_down[l, :, at:at + DOWN_CHUNKS[l][c]]

        parts = {key: first_part(own_piece(*key), order) for key in X_ORDER}
        plans = [
            (
                parts['kv', l, 0], parts['q', l, 0], parts['o', l, 0],
                [parts['g', l, c] for c in range(len(FFN_CHUNKS[l]))],
                [parts['d', l, c] for c in range(len(DOWN_CHUNKS[l]))],
            )
            for l in range(layers)
        ]

        seg_far = send_y(seg_ids)
        x_got = send_y(x_in)
        x_own, x_far = ([p.astype(F32) for p in local_cols(a.reshape(rows, feat), 1)] for a in (x_in, x_got))
        first_half = jnp.where(half_id == 0, seg_ids, seg_far)
        second_half = jnp.where(half_id == 0, seg_far, seg_ids)
        positions = seg_positions(jnp.concatenate([first_half, second_half], axis=1))
        idx = jnp.arange(part_len, dtype=jnp.int32)
        at_own = half_id * part_len
        at_far = (1 - half_id) * part_len
        inv_freq = ROPE_BASE ** (-2.0 * jnp.arange(head_dim // 2, dtype=F32) / head_dim)

        def tables(at):
            pos = lax.dynamic_slice_in_dim(positions, at, part_len, 1)
            hi = jnp.broadcast_to((idx + at)[None, :], pos.shape)
            angles = (pos.astype(F32)[..., None] * inv_freq).reshape(rows, -1)
            return jnp.cos(angles), jnp.sin(angles), (hi - pos)[..., None], hi[..., None], (idx + at)[None, :]

        cos_own, sin_own, lo_own, hi_own, idx_own = tables(at_own)
        cos_far, sin_far, lo_far, hi_far, idx_far = tables(at_far)

        resid = x_own
        shape3 = (micro_n, part_len, -1)
        k_cols = plans[0][0][0].shape[1] // 2
        q_cols = plans[0][1][0].shape[1]
        gate_q = ()
        out = jnp.zeros((rows, feat), F32)
        y_next = send_y(after(plans[0][2][0], x_got))
        for l in range(layers):
            kv_w, q_w, o_w, gu_w, d_w = plans[l]
            gains = [g.astype(F32)[None, :] for g in local_cols(g_attn[l], 0)]
            h_own = norm_pieces(resid, gains)
            if l == 0:
                h_far = norm_pieces(x_far, gains)
            else:
                h_far = send_y(h_own)
            kv_w = spread(kv_w, *gate_q)
            q_w = spread(q_w, *gate_q)
            y_own = y_next
            kv_own = project(h_own, kv_w, cos_own, sin_own, k_cols, head_dim)
            q_own = project(h_own, q_w, cos_own, sin_own, q_cols, head_dim)
            o_w = spread(o_w, q_own)
            kv_far = project(h_far, kv_w, cos_far, sin_far, k_cols, head_dim)
            y_cross = send_y(after(o_w[2], (kv_far, h_far)[l]))
            q_far = project(h_far, q_w, cos_far, sin_far, q_cols, head_dim)
            o_y = (y_own, send_core(y_own), y_cross, send_core(y_cross))
            kv_own, q_own, kv_far, q_far = (a.reshape(shape3) for a in (kv_own, q_own, kv_far, q_far))
            o_far = attention(q_far, kv_own, kv_far, lo_far, hi_far, idx_own, idx_far, head_dim)
            o_got = send_y(o_far).reshape(rows, -1)
            o_own = attention(q_own, kv_own, kv_far, lo_own, hi_own, idx_own, idx_far, head_dim).reshape(rows, -1)
            base = [resid[j] + jnp.dot(o_own, o_w[j], preferred_element_type=F32) for j in range(4)]
            base = lax.optimization_barrier(base)
            resid = [base[j] + jnp.dot(o_got, o_y[j], preferred_element_type=F32) for j in range(4)]

            gains = [g.astype(F32)[None, :] for g in local_cols(g_mlp[l], 0)]
            h_own = norm_pieces(resid, gains)
            h_far = send_y(h_own)
            if l + 1 < layers:
                y_next = send_y(after(plans[l + 1][2][0], h_far))
            act_own = act_far = None
            starts = firsts[l]
            gate = (o_own, h_own)[l]
            pieces = []

            def far_chunk(c, gate, act_far):
                return ffn_chunk(after(h_far, gate), pieces[c], act_far, ffn_cols, starts[c])

            for step in FFN_STEPS[l]:
                c = int(step[1])
                if c == len(pieces):
                    pieces.append(spread(gu_w[c], gate))
                if step[0] == 'f':
                    act_far = far_chunk(c, gate, act_far)
                    gate = act_far
                else:
                    act_own = ffn_chunk(after(h_own, gate), pieces[c], act_own, ffn_cols, starts[c])
                    gate = act_own
            far_sums = {}
            own_sums = {}
            gates = (gate,)
            own_gate = ()
            cols_at = [sum(DOWN_CHUNKS[l][:c]) for c in range(len(d_w))]

            def far_dots(js, c, w4):
                got_here = []
                for j in js:
                    far_sum = jnp.dot(act_far, w4[j], preferred_element_type=F32)
                    far_sums[j, c] = send_y(far_sum)
                    got_here.append(far_sum)
                return tuple(got_here)

            def own_dots(js, c, w4):
                for j in js:
                    dot = jnp.dot(after(act_own, *own_gate), w4[j], preferred_element_type=F32)
                    own_sums[j, c] = lax.optimization_barrier(dot)
                return tuple(own_sums[j, c] for j in js)

            for c, parts_c in enumerate(d_w):
                far_dots((0, 1), c, parts_c)
            spreads = {}
            for step in DOWN_STEPS[l]:
                if step == 'o':
                    gates = sum((own_dots((0, 1), c, parts_c) for c, parts_c in enumerate(d_w)), ())
                    continue
                c = int(step[1])
                if step[0] == 'f':
                    spreads[c] = spread(d_w[c], *gates)
                    own_gate = gates = far_dots((2, 3), c, spreads[c])
                else:
                    gates = own_dots((2, 3), c, spreads[c])
            new_resid = [[] for _ in range(4)]
            for j, c in far_sums:
                width = DOWN_CHUNKS[l][c]
                at = cols_at[c]
                total = resid[j][:, at:at + width] + own_sums[j, c] + after(far_sums[j, c], *gates)
                new_resid[j].append(total)
                if l + 1 == layers:
                    out = lax.dynamic_update_slice_in_dim(out, total, (tok ^ j) * depth + at, 1)
            gate_q = gates
            resid = [jnp.concatenate(new_resid[j], axis=1) for j in range(4)]
        return out.reshape(micro_n, part_len, feat)

    return jax.shard_map(
        layer_pair,
        mesh=mesh,
        in_specs=(act_spec, seg_spec, gain_spec, head_in, head_in, head_in, head_out, gain_spec, ffn_in, ffn_in, ffn_out),
        out_specs=act_spec,
        check_vma=False,
    )
```

```python
import functools

import jax
import jax.numpy as jnp
from jax import lax
from jax.experimental import pallas as pl
from jax.experimental.pallas import tpu as pltpu
from jax.sharding import PartitionSpec as P


NORM_EPS = 1e-5
ROPE_BASE = 10000.0
NEG_BIG = -1e30
F32 = jnp.float32
BF16 = jnp.bfloat16
VMEM_LIMIT = 60 * 1024 * 1024


def seg_positions(seg_rows):
    positions = jnp.arange(seg_rows.shape[-1], dtype=jnp.int32)
    previous = jnp.concatenate([seg_rows[..., :1] - 1, seg_rows[..., :-1]], axis=-1)
    start_at = jnp.where(seg_rows != previous, positions, 0)
    return positions - lax.cummax(start_at, axis=seg_rows.ndim - 1)


def piece_dot(h_ref, piece_refs, whole_ref):
    depth = piece_refs[0].shape[0]
    for j, w_ref in enumerate(piece_refs):
        whole_ref[j * depth:(j + 1) * depth, :] = w_ref[...]
    return jnp.dot(h_ref[...], whole_ref[...], preferred_element_type=F32)


def proj_kernel(rope_tiles, head_dim, h_ref, *refs):
    piece_refs, (cos_ref, sin_ref, out_ref, whole_ref) = refs[:4], refs[4:]
    acc = piece_dot(h_ref, piece_refs, whole_ref)
    half = head_dim // 2

    def roped():
        cos_t, sin_t = cos_ref[...], sin_ref[...]
        for n in range(acc.shape[1] // head_dim):
            lo = n * head_dim
            a, b = acc[:, lo:lo + half], acc[:, lo + half:lo + head_dim]
            out_ref[:, lo:lo + half] = (a * cos_t - b * sin_t).astype(BF16)
            out_ref[:, lo + half:lo + head_dim] = (b * cos_t + a * sin_t).astype(BF16)

    def plain():
        out_ref[...] = acc.astype(BF16)

    if rope_tiles >= 1000:
        roped()
    else:
        tile = pl.program_id(0)
        pl.when(tile < rope_tiles)(roped)
        pl.when(tile >= rope_tiles)(plain)


def project(hidden, pieces, cos_t, sin_t, rope_cols, head_dim, tile=512):
    rows, feat = hidden.shape
    depth, cols = pieces[0].shape
    rope_tiles = 1000 if rope_cols == cols else rope_cols // tile
    return pl.pallas_call(
        functools.partial(proj_kernel, rope_tiles, head_dim),
        grid=(cols // tile,),
        in_specs=[pl.BlockSpec((rows, feat), lambda i: (0, 0))]
        + [pl.BlockSpec((depth, tile), lambda i: (0, i))] * 4
        + [pl.BlockSpec(cos_t.shape, lambda i: (0, 0))] * 2,
        out_specs=pl.BlockSpec((rows, tile), lambda i: (0, i)),
        out_shape=jax.ShapeDtypeStruct((rows, cols), BF16),
        scratch_shapes=[pltpu.VMEM((feat, tile), BF16)],
        compiler_params=pltpu.CompilerParams(vmem_limit_bytes=VMEM_LIMIT),
        cost_estimate=pl.CostEstimate(flops=2 * rows * feat * cols, bytes_accessed=2 * (rows * feat + feat * cols + rows * cols), transcendentals=0),
    )(hidden, *pieces, cos_t, sin_t)


def ffn_kernel(h_ref, *refs):
    out_ref, whole_gate, whole_up = refs[-3:]
    gate = piece_dot(h_ref, refs[0:4], whole_gate)
    up = piece_dot(h_ref, refs[4:8], whole_up)
    out_ref[...] = (gate * jax.nn.sigmoid(gate) * up).astype(BF16)


def ffn_chunk(hidden, pieces, act_buf, total_cols, first_col, tile=256):
    rows, feat = hidden.shape
    depth, both = pieces[0].shape
    cols = both // 2
    steps, base = cols // tile, first_col // tile
    gate_spec = pl.BlockSpec((depth, tile), lambda i: (0, i))
    up_spec = pl.BlockSpec((depth, tile), lambda i: (0, steps + i))
    in_specs = [pl.BlockSpec((rows, feat), lambda i: (0, 0))] + [gate_spec] * 4 + [up_spec] * 4
    operands = [hidden, *pieces, *pieces]
    aliases = {}
    if act_buf is not None:
        in_specs.append(pl.BlockSpec(memory_space=pl.ANY))
        operands.append(act_buf)
        aliases = {9: 0}
    return pl.pallas_call(
        ffn_kernel,
        grid=(steps,),
        in_specs=in_specs,
        out_specs=pl.BlockSpec((rows, tile), lambda i: (0, base + i)),
        out_shape=jax.ShapeDtypeStruct((rows, total_cols), BF16),
        input_output_aliases=aliases,
        scratch_shapes=[pltpu.VMEM((feat, tile), BF16)] * 2,
        compiler_params=pltpu.CompilerParams(vmem_limit_bytes=VMEM_LIMIT),
        cost_estimate=pl.CostEstimate(flops=4 * rows * feat * cols, bytes_accessed=2 * (rows * feat + 2 * feat * cols + rows * cols), transcendentals=rows * cols),
    )(*operands)


def attn_kernel(head_dim, q_ref, ka_ref, va_ref, kb_ref, vb_ref, lo_ref, hi_ref, ia_ref, ib_ref, out_ref):
    lo, hi = lo_ref[0], hi_ref[0]
    ok_a = (ia_ref[...] >= lo) & (ia_ref[...] <= hi)
    ok_b = (ib_ref[...] >= lo) & (ib_ref[...] <= hi)
    dims = (((1,), (1,)), ((), ()))
    scale = head_dim ** -0.5
    for g in range(q_ref.shape[2] // head_dim):
        q = q_ref[0, :, g * head_dim:(g + 1) * head_dim]
        s_a = jnp.where(ok_a, lax.dot_general(q, ka_ref[0], dims, preferred_element_type=F32) * scale, NEG_BIG)
        s_b = jnp.where(ok_b, lax.dot_general(q, kb_ref[0], dims, preferred_element_type=F32) * scale, NEG_BIG)
        top = jnp.maximum(jnp.max(s_a, axis=1, keepdims=True), jnp.max(s_b, axis=1, keepdims=True))
        e_a, e_b = jnp.exp(s_a - top), jnp.exp(s_b - top)
        inv = 1.0 / (jnp.sum(e_a, axis=1, keepdims=True) + jnp.sum(e_b, axis=1, keepdims=True))
        out = jnp.dot((e_a * inv).astype(BF16), va_ref[0], preferred_element_type=F32)
        out = out + jnp.dot((e_b * inv).astype(BF16), vb_ref[0], preferred_element_type=F32)
        out_ref[0, :, g * head_dim:(g + 1) * head_dim] = out.astype(BF16)


def attention(q, kv_a, kv_b, lo, hi, idx_a, idx_b, head_dim):
    micro_n, rows, q_cols = q.shape
    kv_heads = kv_a.shape[2] // head_dim // 2
    group = q_cols // kv_heads
    k_spec = pl.BlockSpec((1, rows, head_dim), lambda m, n: (m, 0, n))
    v_spec = pl.BlockSpec((1, rows, head_dim), lambda m, n: (m, 0, kv_heads + n))
    q_spec = pl.BlockSpec((1, rows, group), lambda m, n: (m, 0, n))
    col_spec = pl.BlockSpec((1, rows, 1), lambda m, n: (m, 0, 0))
    row_spec = pl.BlockSpec((1, rows), lambda m, n: (0, 0))
    return pl.pallas_call(
        functools.partial(attn_kernel, head_dim),
        grid=(micro_n, kv_heads),
        in_specs=[q_spec, k_spec, v_spec, k_spec, v_spec, col_spec, col_spec, row_spec, row_spec],
        out_specs=q_spec,
        out_shape=jax.ShapeDtypeStruct(q.shape, BF16),
        compiler_params=pltpu.CompilerParams(vmem_limit_bytes=VMEM_LIMIT),
        cost_estimate=pl.CostEstimate(flops=16 * micro_n * rows * rows * q_cols, bytes_accessed=8 * micro_n * rows * q_cols, transcendentals=2 * micro_n * rows * rows * q_cols // head_dim),
    )(q, kv_a, kv_a, kv_b, kv_b, lo, hi, idx_a, idx_b)


def after(value, *earlier):
    return lax.optimization_barrier((value, *earlier))[0] if earlier else value


def norm_pieces(pieces, gains):
    feat = sum(p.shape[1] for p in pieces)
    total = sum(jnp.sum(p * p, axis=1, keepdims=True) for p in pieces)
    inv = lax.rsqrt(total / feat + NORM_EPS)
    return jnp.concatenate([(p * inv * g).astype(BF16) for p, g in zip(pieces, gains)], axis=1)


X_ORDER = (
    ('kv', 0, 0), ('q', 0, 0), ('o', 0, 0), ('g', 0, 0), ('g', 0, 1), ('g', 0, 2), ('g', 0, 3),
    ('d', 0, 0), ('d', 0, 1), ('kv', 1, 0), ('q', 1, 0), ('o', 1, 0), ('g', 1, 0), ('g', 1, 1), ('g', 1, 2), ('g', 1, 3), ('g', 1, 4),
    ('d', 1, 0), ('d', 1, 1), ('d', 1, 2),
)


FFN_CHUNKS = ((2048, 2048, 2048, 1024), (2048, 2048, 1536, 1024, 512))
DOWN_CHUNKS = ((512, 384), (384, 256, 256))
FFN_STEPS = (
    ('w0', 'w1', 'f0', 'f1', 'f2', 'w2', 'f3', 'w3'),
    ('w0', 'w1', 'f0', 'f1', 'f2', 'f3', 'f4', 'w2', 'w3', 'w4'),
)
DOWN_STEPS = (('o', 'f0', 'w0', 'f1', 'w1'), ('f0', 'o', 'f1', 'w0', 'w1', 'f2', 'w2'))


def solution(mesh):
    act_spec = P(None, ('rep', 'tok', 'mp'), None)
    seg_spec = P(None, ('rep', 'tok', 'mp'))
    gain_spec = P(None, None)
    head_in = P(None, 'tok', 'mp', None)
    head_out = P(None, 'mp', None, 'tok')
    ffn_in = P(None, 'tok', 'mp')
    ffn_out = P(None, 'mp', 'tok')
    tok_n = mesh.shape['tok']
    over_x = [(i, i ^ 2) for i in range(tok_n)]
    over_core = [(i, i ^ 1) for i in range(tok_n)]

    def send_x(a):
        return lax.ppermute(a, 'tok', over_x)

    def send_core(a):
        return lax.ppermute(a, 'tok', over_core)

    def send_y(a):
        return lax.ppermute(a, 'mp', [(0, 1), (1, 0)])

    def first_part(own, order):
        k = len(order)
        order.append(k)
        return own, send_core(own), send_x(own), k

    def spread(parts, *earlier):
        own, near, cross, _ = parts
        cross = after(cross, *earlier)
        return own, near, cross, send_core(cross)

    def layer_pair(x_in, seg_ids, g_attn, w_q, w_k, w_v, w_o, g_mlp, w_gate, w_up, w_down):
        micro_n, part_len, feat = x_in.shape
        layers, depth = w_q.shape[0], w_q.shape[1]
        head_dim = w_q.shape[3]
        rows = micro_n * part_len
        ffn_cols = w_gate.shape[2]
        tok = lax.axis_index('tok')
        half_id = lax.axis_index('mp')

        def local_cols(a, axis):
            return [lax.dynamic_slice_in_dim(a, (tok ^ j) * depth, depth, axis) for j in range(4)]

        order = []
        firsts = [[sum(w[:c]) for c in range(len(w))] for w in FFN_CHUNKS]

        def own_piece(kind, l, c):
            if kind == 'kv':
                return jnp.concatenate([w_k[l].reshape(depth, -1), w_v[l].reshape(depth, -1)], axis=1)
            if kind == 'q':
                return w_q[l].reshape(depth, -1)
            if kind == 'o':
                return w_o[l].reshape(-1, depth)
            if kind == 'g':
                at = slice(firsts[l][c], firsts[l][c] + FFN_CHUNKS[l][c])
                return jnp.concatenate([w_gate[l, :, at], w_up[l, :, at]], axis=1)
            at = sum(DOWN_CHUNKS[l][:c])
            return w_down[l, :, at:at + DOWN_CHUNKS[l][c]]

        parts = {key: first_part(own_piece(*key), order) for key in X_ORDER}
        plans = [
            (
                parts['kv', l, 0], parts['q', l, 0], parts['o', l, 0],
                [parts['g', l, c] for c in range(len(FFN_CHUNKS[l]))],
                [parts['d', l, c] for c in range(len(DOWN_CHUNKS[l]))],
            )
            for l in range(layers)
        ]

        seg_far = send_y(seg_ids)
        x_got = send_y(x_in)
        x_own, x_far = ([p.astype(F32) for p in local_cols(a.reshape(rows, feat), 1)] for a in (x_in, x_got))
        first_half = jnp.where(half_id == 0, seg_ids, seg_far)
        second_half = jnp.where(half_id == 0, seg_far, seg_ids)
        positions = seg_positions(jnp.concatenate([first_half, second_half], axis=1))
        idx = jnp.arange(part_len, dtype=jnp.int32)
        at_own = half_id * part_len
        at_far = (1 - half_id) * part_len
        inv_freq = ROPE_BASE ** (-2.0 * jnp.arange(head_dim // 2, dtype=F32) / head_dim)

        def tables(at):
            pos = lax.dynamic_slice_in_dim(positions, at, part_len, 1)
            hi = jnp.broadcast_to((idx + at)[None, :], pos.shape)
            angles = (pos.astype(F32)[..., None] * inv_freq).reshape(rows, -1)
            return jnp.cos(angles), jnp.sin(angles), (hi - pos)[..., None], hi[..., None], (idx + at)[None, :]

        cos_own, sin_own, lo_own, hi_own, idx_own = tables(at_own)
        cos_far, sin_far, lo_far, hi_far, idx_far = tables(at_far)

        resid = x_own
        shape3 = (micro_n, part_len, -1)
        k_cols = plans[0][0][0].shape[1] // 2
        q_cols = plans[0][1][0].shape[1]
        gate_q = ()
        out = jnp.zeros((rows, feat), F32)
        y_next = send_y(after(plans[0][2][0], x_got))
        for l in range(layers):
            kv_w, q_w, o_w, gu_w, d_w = plans[l]
            gains = [g.astype(F32)[None, :] for g in local_cols(g_attn[l], 0)]
            h_own = norm_pieces(resid, gains)
            if l == 0:
                h_far = norm_pieces(x_far, gains)
            else:
                h_far = send_y(h_own)
            kv_w = spread(kv_w, *gate_q)
            q_w = spread(q_w, *gate_q)
            y_own = y_next
            kv_own = project(h_own, kv_w, cos_own, sin_own, k_cols, head_dim)
            q_own = project(h_own, q_w, cos_own, sin_own, q_cols, head_dim)
            o_w = spread(o_w, q_own)
            kv_far = project(h_far, kv_w, cos_far, sin_far, k_cols, head_dim)
            y_cross = send_y(after(o_w[2], (kv_far, h_far)[l]))
            q_far = project(h_far, q_w, cos_far, sin_far, q_cols, head_dim)
            o_y = (y_own, send_core(y_own), y_cross, send_core(y_cross))
            kv_own, q_own, kv_far, q_far = (a.reshape(shape3) for a in (kv_own, q_own, kv_far, q_far))
            o_far = attention(q_far, kv_own, kv_far, lo_far, hi_far, idx_own, idx_far, head_dim)
            o_got = send_y(o_far).reshape(rows, -1)
            o_own = attention(q_own, kv_own, kv_far, lo_own, hi_own, idx_own, idx_far, head_dim).reshape(rows, -1)
            base = [resid[j] + jnp.dot(o_own, o_w[j], preferred_element_type=F32) for j in range(4)]
            base = lax.optimization_barrier(base)
            resid = [base[j] + jnp.dot(o_got, o_y[j], preferred_element_type=F32) for j in range(4)]

            gains = [g.astype(F32)[None, :] for g in local_cols(g_mlp[l], 0)]
            h_own = norm_pieces(resid, gains)
            h_far = send_y(h_own)
            if l + 1 < layers:
                y_next = send_y(after(plans[l + 1][2][0], h_far))
            act_own = act_far = None
            starts = firsts[l]
            gate = (o_own, h_own)[l]
            pieces = []

            def far_chunk(c, gate, act_far):
                return ffn_chunk(after(h_far, gate), pieces[c], act_far, ffn_cols, starts[c])

            for step in FFN_STEPS[l]:
                c = int(step[1])
                if c == len(pieces):
                    pieces.append(spread(gu_w[c], gate))
                if step[0] == 'f':
                    act_far = far_chunk(c, gate, act_far)
                    gate = act_far
                else:
                    act_own = ffn_chunk(after(h_own, gate), pieces[c], act_own, ffn_cols, starts[c])
                    gate = act_own
            far_sums = {}
            own_sums = {}
            gates = (gate,)
            own_gate = ()
            cols_at = [sum(DOWN_CHUNKS[l][:c]) for c in range(len(d_w))]

            def far_dots(js, c, w4):
                got_here = []
                for j in js:
                    far_sum = jnp.dot(act_far, w4[j], preferred_element_type=F32)
                    far_sums[j, c] = send_y(far_sum)
                    got_here.append(far_sum)
                return tuple(got_here)

            def own_dots(js, c, w4):
                for j in js:
                    dot = jnp.dot(after(act_own, *own_gate), w4[j], preferred_element_type=F32)
                    own_sums[j, c] = lax.optimization_barrier(dot)
                return tuple(own_sums[j, c] for j in js)

            for c, parts_c in enumerate(d_w):
                far_dots((0, 1), c, parts_c)
            spreads = {}
            for step in DOWN_STEPS[l]:
                if step == 'o':
                    gates = sum((own_dots((0, 1), c, parts_c) for c, parts_c in enumerate(d_w)), ())
                    continue
                c = int(step[1])
                if step[0] == 'f':
                    spreads[c] = spread(d_w[c], *gates)
                    own_gate = gates = far_dots((2, 3), c, spreads[c])
                else:
                    gates = own_dots((2, 3), c, spreads[c])
            new_resid = [[] for _ in range(4)]
            for j, c in far_sums:
                width = DOWN_CHUNKS[l][c]
                at = cols_at[c]
                total = resid[j][:, at:at + width] + own_sums[j, c] + after(far_sums[j, c], *gates)
                new_resid[j].append(total)
                if l + 1 == layers:
                    out = lax.dynamic_update_slice_in_dim(out, total, (tok ^ j) * depth + at, 1)
            gate_q = gates
            resid = [jnp.concatenate(new_resid[j], axis=1) for j in range(4)]
        return out.reshape(micro_n, part_len, feat)

    return jax.shard_map(
        layer_pair,
        mesh=mesh,
        in_specs=(act_spec, seg_spec, gain_spec, head_in, head_in, head_in, head_out, gain_spec, ffn_in, ffn_in, ffn_out),
        out_specs=act_spec,
        check_vma=False,
    )
```
